128 devices in a mesh: row: 8 (over z_hi, x), col: 16 (over z_lo, y, core).
Axes of the slice: x: 4, y: 4, z: 4 (z_hi: 2, z_lo: 2; z = z_hi * 2 + z_lo), core: 2. Of those that a mesh axis runs over, the one named last changes fastest.
Arguments:
- features: bfloat16 [131072, 128], P(('row', 'col')), may hold values from -6 to 6
- pair_index: int32 [2, 16384], P(None, ('row', 'col')), may hold values from -1 to 127, as said below
- bins: int32 [16384, 128, 128], P(('row', 'col')), may hold values from 0 to 8, as said below
- plate_weight: bfloat16 [1024, 128], replicated, may hold values from -0.1875 to 0.1875
- tower_weight: bfloat16 [1024, 128], replicated, may hold values from -0.1875 to 0.1875
- norm_gain: float32 [128], replicated, may hold values from 0.1 to 1.9
- update_in: bfloat16 [256, 128], replicated, may hold values from -0.375 to 0.375
- update_out: bfloat16 [128, 128], replicated, may hold values from -0.5 to 0.5
Outputs:
- updated: bfloat16 [131072, 128], P(('row', 'col'))
The draws below stay inside these ranges and needn't reach their ends.
Inputs may be any that keep to these rules, and one draw needn't show every extreme that they name: `pair_index`: row 0 is a cluster of the meeting device's plate (below 128), row 1 a cluster of its tower (below 64). The 128 slots of one meeting device hold its live pairs first and then -1 in both rows. No cluster pair is live twice on one device. Some device has all 128 slots live. `bins`: 8 marks an atom pair that is no neighbour.
All inputs are finite; a program needn't handle non-finite values.
Results may differ from the reference program's by a relative error of at most 0.008.
Values may be sent and summed in bfloat16 or wider, within the bound.
No kernel may reach another device: no remote copies, remote signals or barrier semaphores. Data moves between devices by JAX's collectives and lax.ppermute only.
A program may use at most 128 MiB of HBM per device.

```python
import jax
import jax.numpy as jnp
from jax import lax

D = 128
CLUSTER = 128
BINS = 8
HOME_DEV = 8
PAIRS_DEV = 128
PLATE = 128
TOWER = 64
CLUSTERS = 1024
N_ROW = 8
N_COL = 16


def draw_pair_index(key, part):
    devices = N_ROW * N_COL
    keys = jax.random.split(jax.random.fold_in(key, 11), devices)
    lowest = max(1, PAIRS_DEV // 8)

    def one_device(inner):
        first, second, third = jax.random.split(inner, 3)
        codes = jax.random.permutation(first, PLATE * TOWER)[:PAIRS_DEV]
        heavy = jax.random.randint(second, (), 0, 6) == 0
        light = jax.random.randint(third, (), lowest, PAIRS_DEV // 3 + 1)
        return (codes, jnp.where(heavy, PAIRS_DEV, light))
    codes, counts = jax.vmap(one_device)(keys)
    forced = jax.random.randint(jax.random.fold_in(key, 12), (), 0, devices)
    counts = jnp.where(jnp.arange(devices) == forced, PAIRS_DEV, counts)
    live = jnp.arange(PAIRS_DEV)[None, :] < counts[:, None]
    plate_idx = jnp.where(live, codes // TOWER, -1)
    tower_idx = jnp.where(live, codes % TOWER, -1)
    return jnp.stack([plate_idx.reshape(-1), tower_idx.reshape(-1)]).astype(jnp.int32)


def draw_bins(key, part):
    total = PAIRS_DEV * N_ROW * N_COL
    raw = jax.random.randint(jax.random.fold_in(key, 21), (total, CLUSTER, CLUSTER), 0, 3 * BINS)
    return jnp.where(raw < BINS, raw, BINS).astype(jnp.int32)


def level_of(rng, dims, cuts, smallest, top_value):
    gain, own = 1.0, jax.random.fold_in(rng, 6)
    for axis_at, parts in cuts:
        heights = jnp.exp(jax.random.uniform(jax.random.fold_in(own, axis_at), (parts,), jnp.float32, smallest / len(cuts), top_value / len(cuts)))
        gain = gain * jnp.repeat(heights, dims[axis_at] // parts).reshape([-1 if axis == axis_at else 1 for axis in range(len(dims))])
    return gain


def scatter_about(stream_key, dims, width, reach, cuts=(), kind=jnp.bfloat16):
    entries = jax.random.normal(stream_key, dims, jnp.float32) * width
    if len(cuts) > 0:
        entries = level_of(stream_key, dims, cuts, -0.22, 0.18) * entries
    return jnp.clip(entries, min=-reach, max=reach).astype(kind)


def setup_inputs(seed: int = 0) -> dict:
    splits = jax.random.split(jax.random.key(seed), 9)
    features = scatter_about(splits[0], (CLUSTERS * CLUSTER, D), 1.0, 6.0, ((0, 128),))
    pair_index = draw_pair_index(jax.random.fold_in(splits[8], 71), 0)
    bins = draw_bins(jax.random.fold_in(splits[8], 71), 0)
    plate_weight = scatter_about(splits[3], (BINS * D, D), (BINS * D) ** -0.5, 0.1875)
    tower_weight = scatter_about(splits[4], (BINS * D, D), (BINS * D) ** -0.5, 0.1875)
    norm_gain = jnp.clip(1.0 + 0.18 * jax.random.normal(splits[5], (D,), jnp.float32), 0.1, 1.9)
    update_in = scatter_about(splits[6], (2 * D, D), (2 * D) ** -0.5, 0.375)
    update_out = scatter_about(splits[7], (D, D), D ** -0.5, 0.5)
    return {"features": features, "pair_index": pair_index, "bins": bins, "plate_weight": plate_weight, "tower_weight": tower_weight, "norm_gain": norm_gain, "update_in": update_in, "update_out": update_out}


def pair_messages(plate, tower, plate_idx, tower_idx, block, plate_weight, tower_weight):
    live = plate_idx >= 0
    plate_at = jnp.maximum(plate_idx, 0).astype(jnp.int32)
    tower_at = jnp.maximum(tower_idx, 0).astype(jnp.int32)
    levels = jnp.arange(BINS, dtype=jnp.int32)
    basis = ((block[:, :, None, :] == levels[None, None, :, None]) & live[:, None, None, None]).astype(jnp.float32)
    far_side = tower[tower_at].astype(jnp.float32)
    near_side = plate[plate_at].astype(jnp.float32)
    near_plate = jnp.einsum('gakb,gbd->gakd', basis, far_side).astype(jnp.bfloat16)
    near_tower = jnp.einsum('gakb,gad->gbkd', basis, near_side).astype(jnp.bfloat16)
    count = block.shape[0]
    to_plate = jnp.dot(near_plate.reshape(count * CLUSTER, BINS * D), plate_weight, preferred_element_type=jnp.float32)
    to_tower = jnp.dot(near_tower.reshape(count * CLUSTER, BINS * D), tower_weight, preferred_element_type=jnp.float32)
    return (plate_at, tower_at, to_plate.reshape(count, CLUSTER, D), to_tower.reshape(count, CLUSTER, D))

def reference(features, pair_index, bins, plate_weight, tower_weight, norm_gain, update_in, update_out):
    grid = features.reshape(N_ROW, N_COL, HOME_DEV, CLUSTER, D)
    group = 8

    def device_step(total, device):
        row_at = device // N_COL
        col_at = device % N_COL
        plate = lax.dynamic_index_in_dim(grid, row_at, 0, keepdims=False).reshape(N_COL * HOME_DEV, CLUSTER, D)
        tower = lax.dynamic_index_in_dim(grid, col_at, 1, keepdims=False).reshape(N_ROW * HOME_DEV, CLUSTER, D)

        def block_step(inner, turn):
            plate_part, tower_part = inner
            start = (device * PAIRS_DEV + turn * group).astype(jnp.int32)
            plate_idx = lax.dynamic_slice_in_dim(pair_index[0], start, group)
            tower_idx = lax.dynamic_slice_in_dim(pair_index[1], start, group)
            block = lax.dynamic_slice_in_dim(bins, start, group, 0)
            plate_at, tower_at, to_plate, to_tower = pair_messages(plate, tower, plate_idx, tower_idx, block, plate_weight, tower_weight)
            plate_part = plate_part.at[plate_at].add(to_plate)
            tower_part = tower_part.at[tower_at].add(to_tower)
            return ((plate_part, tower_part), None)
        start_parts = (jnp.zeros((N_COL * HOME_DEV, CLUSTER, D), jnp.float32), jnp.zeros((N_ROW * HOME_DEV, CLUSTER, D), jnp.float32))
        (plate_part, tower_part), _ = lax.scan(block_step, start_parts, jnp.arange(PAIRS_DEV // group, dtype=jnp.int32))
        plate_round = lax.optimization_barrier(plate_part.astype(jnp.bfloat16)).astype(jnp.float32)
        tower_round = lax.optimization_barrier(tower_part.astype(jnp.bfloat16)).astype(jnp.float32)
        total = total.at[row_at].add(plate_round.reshape(N_COL, HOME_DEV, CLUSTER, D))
        total = total.at[:, col_at].add(tower_round.reshape(N_ROW, HOME_DEV, CLUSTER, D))
        return (total, None)
    start_total = jnp.zeros((N_ROW, N_COL, HOME_DEV, CLUSTER, D), jnp.float32)
    total, _ = lax.scan(device_step, start_total, jnp.arange(N_ROW * N_COL, dtype=jnp.int32))
    incoming = total.reshape(CLUSTERS * CLUSTER, D)
    scale = lax.rsqrt(lax.optimization_barrier(jnp.mean(incoming * incoming, axis=1, keepdims=True)) + 1e-06)
    normed = (incoming * scale * norm_gain[None, :]).astype(jnp.bfloat16)
    joined = jnp.concatenate([features, normed], axis=1)
    hidden = jax.nn.silu(jnp.dot(joined, update_in, preferred_element_type=jnp.float32)).astype(jnp.bfloat16)
    result = features.astype(jnp.float32) + jnp.dot(hidden, update_out, preferred_element_type=jnp.float32)
    return result.astype(jnp.bfloat16)
```

```python
import jax
import jax.numpy as jnp
from jax import lax
from jax.experimental import pallas as pl
from jax.experimental.pallas import tpu as pltpu
from jax.sharding import PartitionSpec as P

D = 128
CLUSTER = 128
BINS = 8
SLOTS = 128
BLOCK = 8
MIB = 1024 * 1024


def live_count(index_ref):
    count = jnp.int32(0)
    for step in (128, 64, 32, 16, 8, 4, 2, 1):
        at = count + step
        inside = at <= SLOTS
        live = index_ref[0, jnp.minimum(at, SLOTS) - 1] >= 0
        count = jnp.where(inside & live, at, count)
    return count


def start_bins(bins_hbm, bins_ref, sems, blocks):
    def start(block, _):
        pltpu.make_async_copy(
            bins_hbm.at[pl.ds(block * BLOCK, BLOCK)],
            bins_ref.at[pl.ds(block * BLOCK, BLOCK)],
            sems.at[block],
        ).start()
        return 0

    lax.fori_loop(0, blocks, start, 0)


def wait_bins(bins_hbm, bins_ref, sems, block):
    pltpu.make_async_copy(
        bins_hbm.at[pl.ds(block * BLOCK, BLOCK)],
        bins_ref.at[pl.ds(block * BLOCK, BLOCK)],
        sems.at[block],
    ).wait()


def basis_of(bins_ref, slot):
    level = bins_ref[slot].astype(jnp.float32).astype(jnp.bfloat16)
    one = jnp.ones((), jnp.bfloat16)
    zero = jnp.zeros((), jnp.bfloat16)
    return [jnp.where(level == jnp.bfloat16(k), one, zero) for k in range(BINS)]


def plate_kernel(index_ref, bins_hbm, tower_ref, weight_ref, out_ref, bins_ref, far_ref, acc_ref, sems):
    count = live_count(index_ref)
    blocks = (count + BLOCK - 1) // BLOCK
    start_bins(bins_hbm, bins_ref, sems, blocks)
    clusters = tower_ref.shape[0] // CLUSTER

    def zero(i, _):
        acc_ref[i] = jnp.zeros((CLUSTER, D), jnp.float32)
        return 0

    lax.fori_loop(0, acc_ref.shape[0], zero, 0)

    def project(i, _):
        rows = tower_ref[pl.ds(i * CLUSTER, CLUSTER), :]
        for k in range(0, BINS, 2):
            both = jnp.dot(
                rows, weight_ref[:, k * D : (k + 2) * D], preferred_element_type=jnp.float32
            ).astype(jnp.bfloat16)
            far_ref[i, k * CLUSTER : (k + 1) * CLUSTER, :] = both[:, :D]
            far_ref[i, (k + 1) * CLUSTER : (k + 2) * CLUSTER, :] = both[:, D:]
        return 0

    lax.fori_loop(0, clusters, project, 0)

    def block_step(block, _):
        wait_bins(bins_hbm, bins_ref, sems, block)

        def pair_step(half, _):
            for u in range(2):
                slot = block * BLOCK + half * 2 + u
                plate_at = index_ref[0, slot]
                plate_at = jnp.where(plate_at < 0, SLOTS, plate_at)
                tower_at = jnp.maximum(index_ref[1, slot], 0)
                basis = jnp.concatenate(basis_of(bins_ref, slot), axis=1)
                message = jnp.dot(basis, far_ref[tower_at], preferred_element_type=jnp.float32)
                acc_ref[plate_at] += message
            return 0

        lax.fori_loop(0, BLOCK // 2, pair_step, 0)
        return 0

    lax.fori_loop(0, blocks, block_step, 0)

    def finish(i, _):
        out_ref[pl.ds(i * CLUSTER, CLUSTER), :] = acc_ref[i].astype(jnp.bfloat16)
        return 0

    lax.fori_loop(0, acc_ref.shape[0] - 1, finish, 0)


def tower_kernel(index_ref, bins_hbm, plate_ref, weight_ref, out_ref, bins_ref, acc_ref, sems):
    count = live_count(index_ref)
    blocks = (count + BLOCK - 1) // BLOCK
    start_bins(bins_hbm, bins_ref, sems, blocks)
    clusters = acc_ref.shape[0] - 1

    def zero(i, _):
        acc_ref[i] = jnp.zeros((D, CLUSTER), jnp.float32)
        return 0

    lax.fori_loop(0, acc_ref.shape[0], zero, 0)

    def block_step(block, _):
        wait_bins(bins_hbm, bins_ref, sems, block)

        def pair_step(half, _):
            nears = []
            for u in range(2):
                slot = block * BLOCK + half * 2 + u
                plate_at = jnp.maximum(index_ref[0, slot], 0)
                rows = plate_ref[pl.ds(pl.multiple_of(plate_at * CLUSTER, CLUSTER), CLUSTER), :]
                flipped = rows.T
                basis = basis_of(bins_ref, slot)
                near = [
                    jnp.dot(
                        flipped,
                        jnp.concatenate(basis[k : k + 2], axis=1),
                        preferred_element_type=jnp.float32,
                    ).astype(jnp.bfloat16)
                    for k in range(0, BINS, 2)
                ]
                nears.append(
                    jnp.concatenate(
                        [part[:, h * CLUSTER : (h + 1) * CLUSTER] for part in near for h in range(2)],
                        axis=0,
                    )
                )
            both = jnp.concatenate(nears, axis=1)
            message = jnp.dot(weight_ref[...], both, preferred_element_type=jnp.float32)
            for u in range(2):
                slot = block * BLOCK + half * 2 + u
                tower_at = index_ref[1, slot]
                tower_at = jnp.where(tower_at < 0, clusters, tower_at)
                acc_ref[tower_at] += message[:, u * CLUSTER : (u + 1) * CLUSTER]
            return 0

        lax.fori_loop(0, BLOCK // 2, pair_step, 0)
        return 0

    lax.fori_loop(0, blocks, block_step, 0)

    def finish(i, _):
        out_ref[pl.ds(i * CLUSTER, CLUSTER), :] = acc_ref[i].T.astype(jnp.bfloat16)
        return 0

    lax.fori_loop(0, clusters, finish, 0)


SMEM = pl.BlockSpec(memory_space=pltpu.SMEM)
VMEM = pl.BlockSpec(memory_space=pltpu.VMEM)
ANY = pl.BlockSpec(memory_space=pl.ANY)


def plate_messages(pair_index, bins, tower, weight, clusters):
    return pl.pallas_call(
        plate_kernel,
        out_shape=jax.ShapeDtypeStruct((clusters * CLUSTER, D), jnp.bfloat16),
        in_specs=[SMEM, ANY, VMEM, VMEM],
        out_specs=VMEM,
        scratch_shapes=[
            pltpu.VMEM((SLOTS, CLUSTER, CLUSTER), jnp.int32),
            pltpu.VMEM((tower.shape[0] // CLUSTER, BINS * CLUSTER, D), jnp.bfloat16),
            pltpu.VMEM((clusters + 1, CLUSTER, D), jnp.float32),
            pltpu.SemaphoreType.DMA((SLOTS // BLOCK,)),
        ],
        compiler_params=pltpu.CompilerParams(vmem_limit_bytes=48 * MIB),
        cost_estimate=pl.CostEstimate(flops=30_000_000_000, bytes_accessed=15_000_000, transcendentals=0),
        name="plate_messages",
    )(pair_index, bins, tower, weight)


def tower_messages(pair_index, bins, plate, weight, clusters):
    return pl.pallas_call(
        tower_kernel,
        out_shape=jax.ShapeDtypeStruct((clusters * CLUSTER, D), jnp.bfloat16),
        in_specs=[SMEM, ANY, VMEM, VMEM],
        out_specs=VMEM,
        scratch_shapes=[
            pltpu.VMEM((SLOTS, CLUSTER, CLUSTER), jnp.int32),
            pltpu.VMEM((clusters + 1, D, CLUSTER), jnp.float32),
            pltpu.SemaphoreType.DMA((SLOTS // BLOCK,)),
        ],
        compiler_params=pltpu.CompilerParams(vmem_limit_bytes=48 * MIB),
        cost_estimate=pl.CostEstimate(flops=30_000_000_000, bytes_accessed=15_000_000, transcendentals=0),
        name="tower_messages",
    )(pair_index, bins, plate, weight)


def from_everyone(value, axis):
    copies = jnp.broadcast_to(value, (lax.axis_size(axis), *value.shape))
    return lax.all_to_all(copies, axis, split_axis=0, concat_axis=0, tiled=True)


def shards(
    features, pair_index, bins, plate_weight, tower_weight, norm_gain, update_in, update_out
):
    plate = lax.all_gather(features, "col", axis=0, tiled=True)
    tower = from_everyone(features, "row").reshape(-1, D)
    plate_cat = plate_weight.reshape(BINS, D, D).transpose(1, 0, 2).reshape(D, BINS * D)
    tower_flip = tower_weight.T
    plate_clusters = plate.shape[0] // CLUSTER
    tower_clusters = tower.shape[0] // CLUSTER
    plate_part = plate_messages(pair_index, bins, tower, plate_cat, plate_clusters)
    plate_back = lax.psum_scatter(plate_part, "col", scatter_dimension=0, tiled=True).astype(
        jnp.float32
    )
    tower_part = tower_messages(pair_index, bins, plate, tower_flip, tower_clusters)
    arrived = lax.all_to_all(
        tower_part.reshape(lax.axis_size("row"), -1, D), "row", split_axis=0, concat_axis=0, tiled=True
    )
    incoming = plate_back + arrived.astype(jnp.float32).sum(axis=0)
    scale = lax.rsqrt(jnp.mean(incoming * incoming, axis=1, keepdims=True) + 1e-06)
    normed = (incoming * scale * norm_gain[None, :]).astype(jnp.bfloat16)
    joined = jnp.concatenate([features, normed], axis=1)
    hidden = jax.nn.silu(jnp.dot(joined, update_in, preferred_element_type=jnp.float32)).astype(
        jnp.bfloat16
    )
    result = features.astype(jnp.float32) + jnp.dot(
        hidden, update_out, preferred_element_type=jnp.float32
    )
    return result.astype(jnp.bfloat16)


def solution(mesh):
    placed = (
        P(("row", "col"), None),
        P(None, ("row", "col")),
        P(("row", "col"), None, None),
        P(),
        P(),
        P(),
        P(),
        P(),
    )
    return jax.shard_map(
        shards, mesh=mesh, in_specs=placed, out_specs=P(("row", "col"), None), check_vma=False
    )
```

```python
import jax
import jax.numpy as jnp
from jax import lax
from jax.experimental import pallas as pl
from jax.experimental.pallas import tpu as pltpu
from jax.sharding import PartitionSpec as P


D = 128
CLUSTER = 128
BINS = 8
SLOTS = 128
BLOCK = 8
HOME = 8
CUT = 5
MIB = 1024 * 1024


def live_count(index_ref):
    count = jnp.int32(0)
    for step in (128, 64, 32, 16, 8, 4, 2, 1):
        at = count + step
        inside = at <= SLOTS
        live = index_ref[0, jnp.minimum(at, SLOTS) - 1] >= 0
        count = jnp.where(inside & live, at, count)
    return count


def basis_of(level):
    one = jnp.ones((), jnp.bfloat16)
    zero = jnp.zeros((), jnp.bfloat16)
    level = level.astype(jnp.float32).astype(jnp.bfloat16)
    return [jnp.where(level == jnp.bfloat16(k), one, zero) for k in range(BINS)]


def plate_kernel(place_ref, index_ref, bins_hbm, *refs):
    blocks_hbm, lines_hbm = refs[:8], refs[8:16]
    (weight_ref, mine_hbm, theirs_hbm, line_hbm, bins_ref, tower_ref, far_ref, acc_ref, out_ref,
     sems, tower_sems, out_sems, line_sems) = refs[16:]
    row, col = place_ref[0], place_ref[1]
    row_z, row_x = row // 4, row % 4
    col_z, col_y, core = col // 8, (col // 2) % 4, col % 2

    def block_copy(j):
        source = ((row_z + 2 - j // 4) % 2) * 4 + (row_x + 4 - j % 4) % 4
        rows = pl.ds(pl.multiple_of(source * 1024, 1024), 1024)
        return pltpu.make_async_copy(blocks_hbm[j], tower_ref.at[rows], tower_sems.at[j])

    def line_copy(j):
        return pltpu.make_async_copy(lines_hbm[j], line_hbm.at[pl.ds(j * 1024, 1024)], line_sems.at[j])

    for j in range(8):
        block_copy(j).start()
    for j in range(8):
        line_copy(j).start()
    count = live_count(index_ref)
    blocks = (count + BLOCK - 1) // BLOCK

    def bins_copy(block):
        part = pl.ds(block * BLOCK, BLOCK)
        return pltpu.make_async_copy(bins_hbm.at[part], bins_ref.at[part], sems.at[block])

    def start(block, _):
        bins_copy(block).start()
        return 0

    lax.fori_loop(0, blocks, start, 0)
    for j in range(8):
        block_copy(j).wait()

    acc_ref[SLOTS] = jnp.zeros((CLUSTER, D), jnp.float32)

    def project(i, _):
        for u in range(8):
            acc_ref[i * 8 + u] = jnp.zeros((CLUSTER, D), jnp.float32)
        rows = tower_ref[pl.ds(i * 4 * CLUSTER, 4 * CLUSTER), :]
        for k in range(0, BINS, 2):
            both = jnp.dot(
                rows, weight_ref[:, k * D : (k + 2) * D], preferred_element_type=jnp.float32
            ).astype(jnp.bfloat16)
            for u in range(4):
                part = both[u * CLUSTER : (u + 1) * CLUSTER]
                far_ref[i * 4 + u, k * CLUSTER : (k + 1) * CLUSTER, :] = part[:, :D]
                far_ref[i * 4 + u, (k + 1) * CLUSTER : (k + 2) * CLUSTER, :] = part[:, D:]
        return 0

    lax.fori_loop(0, tower_ref.shape[0] // (4 * CLUSTER), project, 0)

    def block_step(block, _):
        bins_copy(block).wait()
        for u in range(BLOCK):
            slot = block * BLOCK + u
            plate_at = index_ref[0, slot]
            plate_at = jnp.where(plate_at < 0, SLOTS, plate_at)
            tower_at = jnp.maximum(index_ref[1, slot], 0)
            basis = jnp.concatenate(basis_of(bins_ref[slot]), axis=1)
            message = jnp.dot(basis, far_ref[tower_at], preferred_element_type=jnp.float32)
            acc_ref[plate_at] += message
        return 0

    lax.fori_loop(0, blocks, block_step, 0)

    def out_copy(n):
        j = n % 8
        dest = (theirs_hbm, mine_hbm)[n // 8]
        return pltpu.make_async_copy(
            out_ref.at[pl.ds(n * 1024, 1024)], dest.at[pl.ds(j * 1024, 1024)], out_sems.at[n]
        )

    for n in range(16):
        j = n % 8
        side = 1 - core if n < 8 else core
        home = ((col_z + j % 2) % 2) * 8 + ((col_y + j // 2) % 4) * 2 + side
        for u in range(8):
            at = (n * 8 + u) * CLUSTER
            out_ref[at : at + CLUSTER, :] = acc_ref[home * 8 + u].astype(jnp.bfloat16)
        out_copy(n).start()
    for n in range(16):
        out_copy(n).wait()
    for j in range(8):
        line_copy(j).wait()


def tower_kernel(part, place_ref, index_ref, bins_hbm, mine_hbm, theirs_hbm, weight_ref, *refs):
    out_refs = refs[: 1 if part == 0 else 8]
    bins_ref, plate_ref, acc_ref, near_a, near_b, slot_ref, from_ref, to_ref, sems, plate_sems = refs[len(out_refs) :]
    col = place_ref[1]
    col_z, col_y, core = col // 8, (col // 2) % 4, col % 2

    def block_copy(n):
        j = n % 8
        side = core if n < 8 else 1 - core
        source = ((col_z + 2 - j % 2) % 2) * 8 + ((col_y + 4 - j // 2) % 4) * 2 + side
        rows = pl.ds(pl.multiple_of(source * 1024, 1024), 1024)
        block = (mine_hbm, theirs_hbm)[n // 8].at[pl.ds(j * 1024, 1024)]
        return pltpu.make_async_copy(block, plate_ref.at[rows], plate_sems.at[n])

    for n in range(16):
        block_copy(n).start()
    live = live_count(index_ref)
    spare = acc_ref.shape[0] - 1

    first = CUT * part
    width = CUT if part == 0 else HOME - CUT
    for u in range(BLOCK):
        to_ref[u] = spare

    def pick(i, found):
        tower_at = index_ref[1, i]
        inner = tower_at % HOME
        slot_ref[found] = i
        from_ref[found] = index_ref[0, i]
        to_ref[found + BLOCK] = (tower_at // HOME) * width + inner - first
        return found + jnp.where((inner >= first) & (inner < first + width), 1, 0)

    count = lax.fori_loop(0, live, pick, jnp.int32(0))
    for u in range(BLOCK):
        slot_ref[count + u] = 0
        from_ref[count + u] = 0
        to_ref[count + u + BLOCK] = spare
    blocks = (count + BLOCK - 1) // BLOCK

    def start(block, _):
        for u in range(BLOCK):
            at = block * BLOCK + u
            pltpu.make_async_copy(bins_hbm.at[slot_ref[at]], bins_ref.at[at], sems.at[block]).start()
        return 0

    lax.fori_loop(0, blocks, start, 0)

    def zero(i, _):
        for u in range(8):
            acc_ref[i * 8 + u] = jnp.zeros((D, CLUSTER), jnp.float32)
        return 0

    lax.fori_loop(0, spare // 8, zero, 0)
    acc_ref[spare] = jnp.zeros((D, CLUSTER), jnp.float32)
    near_b[...] = jnp.zeros(near_b.shape, jnp.bfloat16)
    for n in range(16):
        block_copy(n).wait()

    def gather_near(base, near_ref):
        for u in range(BLOCK // 2):
            at = base + u
            rows = plate_ref[pl.ds(pl.multiple_of(from_ref[at] * CLUSTER, CLUSTER), CLUSTER), :]
            flipped = rows.T
            basis = basis_of(bins_ref[at])
            for k in range(0, BINS, 2):
                near = jnp.dot(
                    flipped, jnp.concatenate(basis[k : k + 2], axis=1), preferred_element_type=jnp.float32
                ).astype(jnp.bfloat16)
                for h in range(2):
                    near_ref[
                        u // 2, (k + h) * D : (k + h + 1) * D, (u % 2) * CLUSTER : (u % 2 + 1) * CLUSTER
                    ] = near[:, h * CLUSTER : (h + 1) * CLUSTER]

    def send_on(base, near_ref):
        for pair in range(BLOCK // 4):
            message = jnp.dot(weight_ref[...], near_ref[pair], preferred_element_type=jnp.float32)
            for u in range(2):
                acc_ref[to_ref[base + pair * 2 + u + BLOCK]] += message[:, u * CLUSTER : (u + 1) * CLUSTER]

    def block_step(block, _):
        base = block * BLOCK
        pltpu.make_async_copy(
            bins_hbm.at[pl.ds(0, BLOCK)], bins_ref.at[pl.ds(base, BLOCK)], sems.at[block]
        ).wait()
        gather_near(base, near_a)
        send_on(base - BLOCK // 2, near_b)
        gather_near(base + BLOCK // 2, near_b)
        send_on(base, near_a)
        return 0

    lax.fori_loop(0, blocks, block_step, 0)
    send_on(blocks * BLOCK - BLOCK // 2, near_b)

    row = place_ref[0]
    for j in range(8):
        home = j if part == 0 else ((row // 4 + j // 4) % 2) * 4 + (row % 4 + j % 4) % 4
        out_ref = out_refs[0 if part == 0 else j]
        for u in range(width):
            at = ((j * width if part == 0 else 0) + u) * CLUSTER
            out_ref[at : at + CLUSTER, :] = acc_ref[home * width + u].astype(jnp.bfloat16)


def add_kernel(mine_hbm, theirs_hbm, *refs):
    outs, (mine_ref, theirs_ref, sum_ref, in_sems, out_sems) = refs[:4], refs[4:]
    ins = []
    for j in range(4):
        rows = pl.ds(j * 2048, 2048)
        ins.append(
            (
                pltpu.make_async_copy(mine_hbm.at[rows], mine_ref.at[rows], in_sems.at[0, j]),
                pltpu.make_async_copy(theirs_hbm.at[rows], theirs_ref.at[rows], in_sems.at[1, j]),
            )
        )
    order = (1, 3, 2, 0)
    for j in order:
        for copy in ins[j]:
            copy.start()
    back = []
    for j in order:
        for copy in ins[j]:
            copy.wait()
        rows = pl.ds(j * 2048, 2048)
        total = mine_ref[rows, :].astype(jnp.float32) + theirs_ref[rows, :].astype(jnp.float32)
        sum_ref[rows, :] = total.astype(jnp.bfloat16)
        back.append(pltpu.make_async_copy(sum_ref.at[rows], outs[j], out_sems.at[j]))
        back[-1].start()
    for copy in back:
        copy.wait()


def update_kernel(first_ref, *refs):
    second_refs, refs = refs[:8], refs[8:]
    update_rows(first_ref, second_refs, *refs)


def update_rows(first_ref, second_refs, own_ref, back_a, back_b, back_c, across_ref, features_ref, gain_ref, in_ref, last_ref, out_ref):
    for c in range(8):
        rows = slice(c * CLUSTER, (c + 1) * CLUSTER)
        at = (c if c < CUT else c - CUT) * CLUSTER
        flipped = jnp.zeros((D, CLUSTER), jnp.float32)
        for r in range(8):
            arrived = first_ref[r, at : at + CLUSTER, :] if c < CUT else second_refs[r][at : at + CLUSTER, :]
            flipped += arrived.astype(jnp.float32)
        incoming = flipped.T
        for ref in (own_ref, back_a, back_b, back_c, across_ref):
            incoming += ref[rows, :].astype(jnp.float32)
        scale = lax.rsqrt(jnp.mean(incoming * incoming, axis=1, keepdims=True) + 1e-06)
        normed = (incoming * scale * gain_ref[...]).astype(jnp.bfloat16)
        features = features_ref[rows, :]
        mixed = jnp.dot(
            jnp.concatenate([features, normed], axis=1), in_ref[...], preferred_element_type=jnp.float32
        )
        hidden = (mixed / (1.0 + jnp.exp(-mixed))).astype(jnp.bfloat16)
        change = jnp.dot(hidden, last_ref[...], preferred_element_type=jnp.float32)
        out_ref[rows, :] = (features.astype(jnp.float32) + change).astype(jnp.bfloat16)


SMEM = pl.BlockSpec(memory_space=pltpu.SMEM)
VMEM = pl.BlockSpec(memory_space=pltpu.VMEM)
HBM = pl.BlockSpec(memory_space=pltpu.HBM)
PARAMS = pltpu.CompilerParams(vmem_limit_bytes=50 * MIB)


def cost(flops, data):
    return pl.CostEstimate(flops=flops, bytes_accessed=data, transcendentals=0)


def plate_messages(place, pair_index, bins, blocks, lines, weight):
    half = jax.ShapeDtypeStruct((8192, D), jnp.bfloat16)
    return pl.pallas_call(
        plate_kernel,
        out_shape=(half, half, half),
        in_specs=[SMEM, SMEM, HBM, *[HBM] * 16, VMEM],
        out_specs=(HBM, HBM, HBM),
        scratch_shapes=[
            pltpu.VMEM((SLOTS, CLUSTER, CLUSTER), jnp.int32),
            pltpu.VMEM((8192, D), jnp.bfloat16),
            pltpu.VMEM((64, BINS * CLUSTER, D), jnp.bfloat16),
            pltpu.VMEM((SLOTS + 1, CLUSTER, D), jnp.float32),
            pltpu.VMEM((16384, D), jnp.bfloat16),
            pltpu.SemaphoreType.DMA((SLOTS // BLOCK,)),
            pltpu.SemaphoreType.DMA((8,)),
            pltpu.SemaphoreType.DMA((16,)),
            pltpu.SemaphoreType.DMA((8,)),
        ],
        compiler_params=PARAMS,
        cost_estimate=cost(25_000_000_000, 15_000_000),
        name="plate_messages",
    )(place, pair_index, bins, *blocks, *lines, weight)


def tower_messages(part, place, pair_index, bins, mine, theirs, weight):
    clusters = 8 * (CUT if part == 0 else HOME - CUT)
    outs = 1 if part == 0 else 8
    near = pltpu.VMEM((BLOCK // 4, BINS * D, 2 * CLUSTER), jnp.bfloat16)
    return pl.pallas_call(
        lambda *refs: tower_kernel(part, *refs),
        out_shape=[jax.ShapeDtypeStruct((clusters * CLUSTER // outs, D), jnp.bfloat16)] * outs,
        in_specs=[SMEM, SMEM, HBM, HBM, HBM, VMEM],
        out_specs=[VMEM] * outs,
        scratch_shapes=[
            pltpu.VMEM((SLOTS, CLUSTER, CLUSTER), jnp.int32),
            pltpu.VMEM((16384, D), jnp.bfloat16),
            pltpu.VMEM((clusters + 1, D, CLUSTER), jnp.float32),
            near,
            near,
            pltpu.SMEM((SLOTS + BLOCK,), jnp.int32),
            pltpu.SMEM((SLOTS + BLOCK,), jnp.int32),
            pltpu.SMEM((SLOTS + 2 * BLOCK,), jnp.int32),
            pltpu.SemaphoreType.DMA((SLOTS // BLOCK,)),
            pltpu.SemaphoreType.DMA((16,)),
        ],
        compiler_params=pltpu.CompilerParams(vmem_limit_bytes=60 * MIB),
        cost_estimate=cost(15_000_000_000, 10_000_000),
    )(place, pair_index, bins, mine, theirs, weight)


def core_sum(mine, theirs):
    return pl.pallas_call(
        add_kernel,
        out_shape=tuple(jax.ShapeDtypeStruct((2048, D), jnp.bfloat16) for _ in range(4)),
        in_specs=[HBM, HBM],
        out_specs=tuple(HBM for _ in range(4)),
        scratch_shapes=[
            pltpu.VMEM((8192, D), jnp.bfloat16),
            pltpu.VMEM((8192, D), jnp.bfloat16),
            pltpu.VMEM((8192, D), jnp.bfloat16),
            pltpu.SemaphoreType.DMA((2, 4)),
            pltpu.SemaphoreType.DMA((4,)),
        ],
        compiler_params=PARAMS,
        cost_estimate=cost(2_000_000_000, 6_000_000),
        name="core_sum",
    )(mine, theirs)


def update(first, second, own_rows, across, features, gain, update_in, update_out):
    return pl.pallas_call(
        update_kernel,
        out_shape=jax.ShapeDtypeStruct((1024, D), jnp.bfloat16),
        grid=(1,),
        in_specs=[VMEM] * 9 + [pl.BlockSpec((1024, D), lambda i: (0, 0))] * 4 + [VMEM] * 5,
        out_specs=VMEM,
        compiler_params=PARAMS,
        cost_estimate=cost(3_000_000_000, 4_000_000),
        name="update",
    )(first, *second, *own_rows, across, features, gain, update_in, update_out)


def along_col(value, dz, dy):
    pairs = [
        (z * 8 + y * 2 + c, ((z + dz) % 2) * 8 + ((y + dy) % 4) * 2 + c)
        for z in range(2)
        for y in range(4)
        for c in range(2)
    ]
    return lax.ppermute(value, "col", pairs)


def along_row(value, dz, dx):
    pairs = [(z * 4 + x, ((z + dz) % 2) * 4 + (x + dx) % 4) for z in range(2) for x in range(4)]
    return lax.ppermute(value, "row", pairs)


def to_other_core(value):
    return lax.ppermute(value, "col", [(i, i ^ 1) for i in range(16)])


def over_rows(part):
    return lax.all_to_all(
        part.reshape(8, -1, D), "row", split_axis=0, concat_axis=0, tiled=True
    )


def layer(
    features, pair_index, bins, plate_weight, tower_weight, norm_gain, update_in, update_out
):
    place = jnp.stack([lax.axis_index("row"), lax.axis_index("col")]).astype(jnp.int32)
    plate_cat = plate_weight.reshape(BINS, D, D).transpose(1, 0, 2).reshape(D, BINS * D)
    tower_flip = tower_weight.T
    row_far = along_row(features, 1, 0)
    col_far = along_col(features, 1, 0)
    row_near = [along_row(features, 0, d) for d in (1, 3)]
    col_near = [along_col(features, 0, d) for d in (1, 3)]
    row_more = [along_row(row_far, 0, d) for d in (1, 3)]
    col_more = [along_col(col_far, 0, d) for d in (1, 3)]
    row_near.append(along_row(row_near[0], 0, 1))
    col_near.append(along_col(col_near[0], 0, 1))
    row_more.append(along_row(row_more[1], 0, 3))
    col_more.append(along_col(col_more[1], 0, 3))
    tower_blocks = [features, row_near[0], row_near[2], row_near[1], row_far, row_more[0], row_more[2], row_more[1]]
    lines = [features, col_far, col_near[0], col_more[0], col_near[2], col_more[2], col_near[1], col_more[1]]
    part_mine, part_theirs, plate_mine = plate_messages(
        place, pair_index, bins, tower_blocks, lines, plate_cat
    )
    part_back = to_other_core(part_theirs)
    plate_theirs = to_other_core(plate_mine)
    first = tower_messages(0, place, pair_index, bins, plate_mine, plate_theirs, tower_flip)
    own, *sums = core_sum(part_mine, part_back)
    back = [along_col(sums[d - 1], 0, d) for d in (1, 3, 2)]
    second = tower_messages(1, place, pair_index, bins, plate_mine, plate_theirs, tower_flip)
    first_back = over_rows(first[0])
    second_back = [along_row(second[j], j // 4, j % 4) for j in (6, 5, 7, 4, 2, 1, 3)]
    far = own[1024:].astype(jnp.float32)
    for part in back:
        far = far + part[1024:].astype(jnp.float32)
    far = far.astype(jnp.bfloat16)
    across = along_col(far, 1, 0)
    return update(
        first_back, [second[0], *second_back], [own, *back], across, features, norm_gain.reshape(1, D), update_in, update_out
    )


def solution(mesh):
    placed = (
        P(("row", "col"), None),
        P(None, ("row", "col")),
        P(("row", "col"), None, None),
        P(),
        P(),
        P(),
        P(),
        P(),
    )
    return jax.shard_map(layer, mesh=mesh, in_specs=placed, out_specs=P(("row", "col"), None), check_vma=False)
```

```python
import jax
import jax.numpy as jnp
from jax import lax
from jax.experimental import pallas as pl
from jax.experimental.pallas import tpu as pltpu
from jax.sharding import PartitionSpec as P


D = 128
CLUSTER = 128
BINS = 8
SLOTS = 128
BLOCK = 8
HOME = 8
CUT = 5
MIB = 1024 * 1024


def live_count(index_ref):
    count = jnp.int32(0)
    for step in (128, 64, 32, 16, 8, 4, 2, 1):
        at = count + step
        inside = at <= SLOTS
        live = index_ref[0, jnp.minimum(at, SLOTS) - 1] >= 0
        count = jnp.where(inside & live, at, count)
    return count


def basis_of(level):
    one = jnp.ones((), jnp.bfloat16)
    zero = jnp.zeros((), jnp.bfloat16)
    level = level.astype(jnp.float32).astype(jnp.bfloat16)
    return [jnp.where(level == jnp.bfloat16(k), one, zero) for k in range(BINS)]


def plate_kernel(index_ref, bins_hbm, *refs):
    blocks_hbm, lines_hbm = refs[:8], refs[8:16]
    (weight_ref, mine_hbm, theirs_hbm, line_hbm, bins_ref, tower_ref, far_ref, acc_ref, out_ref,
     line_ref, sems, tower_sems, out_sems, line_sems) = refs[16:]
    row, col = index_ref[0, SLOTS], index_ref[1, SLOTS]
    row_z, row_x = row // 4, row % 4
    col_z, col_y, core = col // 8, (col // 2) % 4, col % 2

    def block_copy(j):
        source = ((row_z + 2 - j // 4) % 2) * 4 + (row_x + 4 - j % 4) % 4
        rows = pl.ds(pl.multiple_of(source * 1024, 1024), 1024)
        return pltpu.make_async_copy(blocks_hbm[j], tower_ref.at[rows], tower_sems.at[j])

    def line_copy(j):
        return pltpu.make_async_copy(lines_hbm[j], line_ref.at[pl.ds(j * 1024, 1024)], line_sems.at[j])

    line_out = pltpu.make_async_copy(line_ref, line_hbm, line_sems.at[8])

    for j in range(8):
        block_copy(j).start()
    for j in range(8):
        line_copy(j).start()
    count = live_count(index_ref)
    blocks = (count + BLOCK - 1) // BLOCK

    def bins_copy(block):
        part = pl.ds(block * BLOCK, BLOCK)
        return pltpu.make_async_copy(bins_hbm.at[part], bins_ref.at[part], sems.at[block])

    def start(block, _):
        bins_copy(block).start()
        return 0

    lax.fori_loop(0, blocks, start, 0)
    acc_ref[SLOTS] = jnp.zeros((CLUSTER, D), jnp.float32)

    def project(source, _):
        j = ((row_z + 2 - source // 4) % 2) * 4 + (row_x + 4 - source % 4) % 4
        at = pl.multiple_of(source * 1024, 1024)
        pltpu.make_async_copy(blocks_hbm[0], tower_ref.at[pl.ds(at, 1024)], tower_sems.at[j]).wait()
        for u in range(16):
            acc_ref[source * 16 + u] = jnp.zeros((CLUSTER, D), jnp.float32)
        for half in range(2):
            rows = tower_ref[pl.ds(at + half * 512, 512), :]
            for k in range(0, BINS, 2):
                both = jnp.dot(
                    rows, weight_ref[:, k * D : (k + 2) * D], preferred_element_type=jnp.float32
                ).astype(jnp.bfloat16)
                for u in range(4):
                    part = both[u * CLUSTER : (u + 1) * CLUSTER]
                    to = source * 8 + half * 4 + u
                    far_ref[to, k * CLUSTER : (k + 1) * CLUSTER, :] = part[:, :D]
                    far_ref[to, (k + 1) * CLUSTER : (k + 2) * CLUSTER, :] = part[:, D:]
        return 0

    lax.fori_loop(0, 8, project, 0)
    for j in range(8):
        line_copy(j).wait()
    line_out.start()

    def block_step(block, _):
        bins_copy(block).wait()
        for u in range(BLOCK):
            slot = block * BLOCK + u
            plate_at = index_ref[0, slot]
            plate_at = jnp.where(plate_at < 0, SLOTS, plate_at)
            tower_at = jnp.maximum(index_ref[1, slot], 0)
            basis = jnp.concatenate(basis_of(bins_ref[slot]), axis=1)
            message = jnp.dot(basis, far_ref[tower_at], preferred_element_type=jnp.float32)
            acc_ref[plate_at] += message
        return 0

    lax.fori_loop(0, blocks, block_step, 0)

    def out_copy(n):
        j = n % 8
        dest = (theirs_hbm, mine_hbm)[n // 8]
        return pltpu.make_async_copy(
            out_ref.at[pl.ds(n * 1024, 1024)], dest.at[pl.ds(j * 1024, 1024)], out_sems.at[n]
        )

    for n in range(16):
        j = n % 8
        side = 1 - core if n < 8 else core
        home = ((col_z + j % 2) % 2) * 8 + ((col_y + j // 2) % 4) * 2 + side
        for u in range(8):
            at = (n * 8 + u) * CLUSTER
            out_ref[at : at + CLUSTER, :] = acc_ref[home * 8 + u].astype(jnp.bfloat16)
        out_copy(n).start()
    for n in range(16):
        out_copy(n).wait()
    line_out.wait()


def tower_kernel(part, index_ref, bins_hbm, mine_hbm, theirs_hbm, weight_ref, *refs):
    out_refs = refs[: 1 if part == 0 else 4]
    bins_ref, plate_ref, acc_ref, near_a, near_b, slot_ref, from_ref, to_ref, sems, plate_sems = refs[len(out_refs) :]
    col = index_ref[1, SLOTS]
    col_z, col_y, core = col // 8, (col // 2) % 4, col % 2

    def block_copy(n):
        j = n % 8
        side = core if n < 8 else 1 - core
        source = ((col_z + 2 - j % 2) % 2) * 8 + ((col_y + 4 - j // 2) % 4) * 2 + side
        rows = pl.ds(pl.multiple_of(source * 1024, 1024), 1024)
        block = (mine_hbm, theirs_hbm)[n // 8].at[pl.ds(j * 1024, 1024)]
        return pltpu.make_async_copy(block, plate_ref.at[rows], plate_sems.at[n])

    for n in range(16):
        block_copy(n).start()
    live = live_count(index_ref)
    spare = acc_ref.shape[0] - 1

    first = CUT * part
    width = CUT if part == 0 else HOME - CUT
    for u in range(BLOCK):
        to_ref[u] = spare

    def pick(i, found):
        for u in range(BLOCK):
            slot = i * BLOCK + u
            tower_at = index_ref[1, slot]
            inner = tower_at % HOME
            slot_ref[found] = slot
            from_ref[found] = index_ref[0, slot]
            to_ref[found + BLOCK] = (tower_at // HOME) * width + inner - first
            mine = (tower_at >= 0) & (inner >= first) & (inner < first + width)
            found = found + jnp.where(mine, 1, 0)
        return found

    count = lax.fori_loop(0, (live + BLOCK - 1) // BLOCK, pick, jnp.int32(0))
    for u in range(BLOCK):
        slot_ref[count + u] = 0
        from_ref[count + u] = 0
        to_ref[count + u + BLOCK] = spare
    blocks = (count + BLOCK - 1) // BLOCK

    def start(block, _):
        for u in range(BLOCK):
            at = block * BLOCK + u
            pltpu.make_async_copy(bins_hbm.at[slot_ref[at]], bins_ref.at[at], sems.at[block]).start()
        return 0

    lax.fori_loop(0, blocks, start, 0)

    def zero(i, _):
        for u in range(8):
            acc_ref[i * 8 + u] = jnp.zeros((D, CLUSTER), jnp.float32)
        return 0

    lax.fori_loop(0, spare // 8, zero, 0)
    acc_ref[spare] = jnp.zeros((D, CLUSTER), jnp.float32)
    near_b[...] = jnp.zeros(near_b.shape, jnp.bfloat16)
    for n in range(16):
        block_copy(n).wait()

    def gather_near(base, near_ref):
        for u in range(BLOCK // 2):
            at = base + u
            rows = plate_ref[pl.ds(pl.multiple_of(from_ref[at] * CLUSTER, CLUSTER), CLUSTER), :]
            flipped = rows.T
            basis = basis_of(bins_ref[at])
            for k in range(0, BINS, 2):
                near = jnp.dot(
                    flipped, jnp.concatenate(basis[k : k + 2], axis=1), preferred_element_type=jnp.float32
                ).astype(jnp.bfloat16)
                for h in range(2):
                    near_ref[
                        u // 2, (k + h) * D : (k + h + 1) * D, (u % 2) * CLUSTER : (u % 2 + 1) * CLUSTER
                    ] = near[:, h * CLUSTER : (h + 1) * CLUSTER]

    def send_on(base, near_ref):
        for pair in range(BLOCK // 4):
            message = jnp.dot(weight_ref[...], near_ref[pair], preferred_element_type=jnp.float32)
            for u in range(2):
                acc_ref[to_ref[base + pair * 2 + u + BLOCK]] += message[:, u * CLUSTER : (u + 1) * CLUSTER]

    def block_step(block, _):
        base = block * BLOCK
        pltpu.make_async_copy(
            bins_hbm.at[pl.ds(0, BLOCK)], bins_ref.at[pl.ds(base, BLOCK)], sems.at[block]
        ).wait()
        gather_near(base, near_a)
        send_on(base - BLOCK // 2, near_b)
        gather_near(base + BLOCK // 2, near_b)
        send_on(base, near_a)
        return 0

    lax.fori_loop(0, blocks, block_step, 0)
    send_on(blocks * BLOCK - BLOCK // 2, near_b)

    row = index_ref[0, SLOTS]
    for j in range(8):
        home = j if part == 0 else ((row // 4 + j // 4) % 2) * 4 + (row % 4 + j % 4) % 4
        out_ref = out_refs[0 if part == 0 else j % 4]
        for u in range(width):
            at = ((j if part == 0 else j // 4) * width + u) * CLUSTER
            out_ref[at : at + CLUSTER, :] = acc_ref[home * width + u].astype(jnp.bfloat16)


def add_kernel(mine_hbm, theirs_hbm, *refs):
    outs, (mine_ref, theirs_ref, sum_ref, in_sems, out_sems) = refs[:4], refs[4:]
    ins = []
    for j in range(4):
        rows = pl.ds(j * 2048, 2048)
        ins.append(
            (
                pltpu.make_async_copy(mine_hbm.at[rows], mine_ref.at[rows], in_sems.at[0, j]),
                pltpu.make_async_copy(theirs_hbm.at[rows], theirs_ref.at[rows], in_sems.at[1, j]),
            )
        )
    order = (1, 3, 2, 0)
    for j in order:
        for copy in ins[j]:
            copy.start()
    back = []
    for j in order:
        for copy in ins[j]:
            copy.wait()
        rows = pl.ds(j * 2048, 2048)
        total = mine_ref[rows, :].astype(jnp.float32) + theirs_ref[rows, :].astype(jnp.float32)
        sum_ref[rows, :] = total.astype(jnp.bfloat16)
        back.append(pltpu.make_async_copy(sum_ref.at[rows], outs[j], out_sems.at[j]))
        back[-1].start()
    for copy in back:
        copy.wait()


def updated_rows(flipped, rows, side_refs, features_ref, gain_ref, in_ref, last_ref):
    incoming = flipped.T
    for ref in side_refs:
        incoming += ref[rows, :].astype(jnp.float32)
    scale = lax.rsqrt(jnp.mean(incoming * incoming, axis=1, keepdims=True) + 1e-06)
    normed = (incoming * scale * gain_ref[...]).astype(jnp.bfloat16)
    features = features_ref[rows, :]
    mixed = jnp.dot(
        jnp.concatenate([features, normed], axis=1), in_ref[...], preferred_element_type=jnp.float32
    )
    hidden = (mixed / (1.0 + jnp.exp(-mixed))).astype(jnp.bfloat16)
    change = jnp.dot(hidden, last_ref[...], preferred_element_type=jnp.float32)
    return (features.astype(jnp.float32) + change).astype(jnp.bfloat16)


def early_kernel(arrived_ref, *refs):
    side_refs, (features_ref, gain_ref, in_ref, last_ref, out_hbm, out_ref, sem) = refs[:5], refs[5:]
    for c in range(CUT):
        rows = slice(c * CLUSTER, (c + 1) * CLUSTER)
        flipped = arrived_ref[0, rows, :].astype(jnp.float32)
        for r in range(1, 8):
            flipped += arrived_ref[r, rows, :].astype(jnp.float32)
        out_ref[rows, :] = updated_rows(flipped, rows, side_refs, features_ref, gain_ref, in_ref, last_ref)
    copy = pltpu.make_async_copy(out_ref, out_hbm.at[pl.ds(0, CUT * CLUSTER)], sem)
    copy.start()
    copy.wait()


def late_kernel(early_hbm, *refs):
    arrived_refs, side_refs, refs = refs[:5], refs[5:10], refs[10:]
    features_ref, gain_ref, in_ref, last_ref, out_hbm, out_ref, sem = refs
    for c in range(HOME - CUT):
        at = slice(c * CLUSTER, (c + 1) * CLUSTER)
        rows = slice((CUT + c) * CLUSTER, (CUT + c + 1) * CLUSTER)
        flipped = arrived_refs[0][at, :].astype(jnp.float32)
        for r in range(1, 5):
            flipped += arrived_refs[r][at, :].astype(jnp.float32)
        out_ref[at, :] = updated_rows(flipped, rows, side_refs, features_ref, gain_ref, in_ref, last_ref)
    copy = pltpu.make_async_copy(out_ref, out_hbm.at[pl.ds(CUT * CLUSTER, (HOME - CUT) * CLUSTER)], sem)
    copy.start()
    copy.wait()


SMEM = pl.BlockSpec(memory_space=pltpu.SMEM)
VMEM = pl.BlockSpec(memory_space=pltpu.VMEM)
HBM = pl.BlockSpec(memory_space=pltpu.HBM)
PARAMS = pltpu.CompilerParams(vmem_limit_bytes=50 * MIB)


def cost(flops, data):
    return pl.CostEstimate(flops=flops, bytes_accessed=data, transcendentals=0)


def plate_messages(pair_index, bins, blocks, lines, weight):
    half = jax.ShapeDtypeStruct((8192, D), jnp.bfloat16)
    return pl.pallas_call(
        plate_kernel,
        out_shape=(half, half, half),
        in_specs=[SMEM, HBM, *[HBM] * 16, VMEM],
        out_specs=(HBM, HBM, HBM),
        scratch_shapes=[
            pltpu.VMEM((SLOTS, CLUSTER, CLUSTER), jnp.int32),
            pltpu.VMEM((8192, D), jnp.bfloat16),
            pltpu.VMEM((64, BINS * CLUSTER, D), jnp.bfloat16),
            pltpu.VMEM((SLOTS + 1, CLUSTER, D), jnp.float32),
            pltpu.VMEM((16384, D), jnp.bfloat16),
            pltpu.VMEM((8192, D), jnp.bfloat16),
            pltpu.SemaphoreType.DMA((SLOTS // BLOCK,)),
            pltpu.SemaphoreType.DMA((8,)),
            pltpu.SemaphoreType.DMA((16,)),
            pltpu.SemaphoreType.DMA((9,)),
        ],
        compiler_params=PARAMS,
        cost_estimate=cost(25_000_000_000, 15_000_000),
        name="plate_messages",
    )(pair_index, bins, *blocks, *lines, weight)


def tower_messages(part, pair_index, bins, mine, theirs, weight):
    clusters = 8 * (CUT if part == 0 else HOME - CUT)
    outs = 1 if part == 0 else 4
    near = pltpu.VMEM((BLOCK // 4, BINS * D, 2 * CLUSTER), jnp.bfloat16)
    return pl.pallas_call(
        lambda *refs: tower_kernel(part, *refs),
        out_shape=[jax.ShapeDtypeStruct((clusters * CLUSTER // outs, D), jnp.bfloat16)] * outs,
        in_specs=[SMEM, HBM, HBM, HBM, VMEM],
        out_specs=[VMEM] * outs,
        scratch_shapes=[
            pltpu.VMEM((SLOTS, CLUSTER, CLUSTER), jnp.int32),
            pltpu.VMEM((16384, D), jnp.bfloat16),
            pltpu.VMEM((clusters + 1, D, CLUSTER), jnp.float32),
            near,
            near,
            pltpu.SMEM((SLOTS + BLOCK,), jnp.int32),
            pltpu.SMEM((SLOTS + BLOCK,), jnp.int32),
            pltpu.SMEM((SLOTS + 2 * BLOCK,), jnp.int32),
            pltpu.SemaphoreType.DMA((SLOTS // BLOCK,)),
            pltpu.SemaphoreType.DMA((16,)),
        ],
        compiler_params=pltpu.CompilerParams(vmem_limit_bytes=60 * MIB),
        cost_estimate=cost(15_000_000_000, 10_000_000),
    )(pair_index, bins, mine, theirs, weight)


def core_sum(mine, theirs):
    return pl.pallas_call(
        add_kernel,
        out_shape=tuple(jax.ShapeDtypeStruct((2048, D), jnp.bfloat16) for _ in range(4)),
        in_specs=[HBM, HBM],
        out_specs=tuple(HBM for _ in range(4)),
        scratch_shapes=[
            pltpu.VMEM((8192, D), jnp.bfloat16),
            pltpu.VMEM((8192, D), jnp.bfloat16),
            pltpu.VMEM((8192, D), jnp.bfloat16),
            pltpu.SemaphoreType.DMA((2, 4)),
            pltpu.SemaphoreType.DMA((4,)),
        ],
        compiler_params=PARAMS,
        cost_estimate=cost(2_000_000_000, 6_000_000),
        name="core_sum",
    )(mine, theirs)


def update(part, arrived, own_rows, across, features, gain, update_in, update_out):
    rows = (CUT if part == 0 else HOME - CUT) * CLUSTER
    return pl.pallas_call(
        early_kernel if part == 0 else late_kernel,
        out_shape=jax.ShapeDtypeStruct((1024, D), jnp.bfloat16),
        grid=(1,),
        in_specs=([HBM] + [pl.BlockSpec((rows, D), lambda i: (0, 0))] * 5 if part else [VMEM])
        + [pl.BlockSpec((1024, D), lambda i: (0, 0))] * 4
        + [VMEM] * 5,
        out_specs=HBM,
        scratch_shapes=[pltpu.VMEM((rows, D), jnp.bfloat16), pltpu.SemaphoreType.DMA(())],
        input_output_aliases={0: 0} if part else {},
        compiler_params=pltpu.CompilerParams(vmem_limit_bytes=12 * MIB),
        cost_estimate=cost(2_000_000_000, 4_000_000),
    )(*arrived, *own_rows, across, features, gain, update_in, update_out)


def along_col(value, dz, dy):
    pairs = [
        (z * 8 + y * 2 + c, ((z + dz) % 2) * 8 + ((y + dy) % 4) * 2 + c)
        for z in range(2)
        for y in range(4)
        for c in range(2)
    ]
    return lax.ppermute(value, "col", pairs)


def along_row(value, dz, dx):
    pairs = [(z * 4 + x, ((z + dz) % 2) * 4 + (x + dx) % 4) for z in range(2) for x in range(4)]
    return lax.ppermute(value, "row", pairs)


def to_other_core(value):
    return lax.ppermute(value, "col", [(i, i ^ 1) for i in range(16)])


def over_rows(part):
    return lax.all_to_all(
        part.reshape(8, -1, D), "row", split_axis=0, concat_axis=0, tiled=True
    )


def layer(
    features, pair_index, bins, plate_weight, tower_weight, norm_gain, update_in, update_out
):
    place = jnp.stack([lax.axis_index("row"), lax.axis_index("col")]).astype(jnp.int32)
    table = jnp.concatenate([pair_index, jnp.broadcast_to(place[:, None], (2, SLOTS))], axis=1)
    plate_cat = plate_weight.reshape(BINS, D, D).transpose(1, 0, 2).reshape(D, BINS * D)
    tower_flip = tower_weight.T
    row_far = along_row(features, 1, 0)
    col_far = along_col(features, 1, 0)
    row_near = [along_row(features, 0, d) for d in (1, 3)]
    col_near = [along_col(features, 0, d) for d in (1, 3)]
    row_more = [along_row(row_far, 0, d) for d in (1, 3)]
    col_more = [along_col(col_far, 0, d) for d in (1, 3)]
    row_near.append(along_row(row_near[0], 0, 1))
    col_near.append(along_col(col_near[0], 0, 1))
    row_more.append(along_row(row_far, 0, 2))
    col_more.append(along_col(col_far, 0, 2))
    tower_blocks = [features, row_near[0], row_near[2], row_near[1], row_far, row_more[0], row_more[2], row_more[1]]
    lines = [features, col_far, col_near[0], col_more[0], col_near[2], col_more[2], col_near[1], col_more[1]]
    part_mine, part_theirs, plate_mine = plate_messages(
        table, bins, tower_blocks, lines, plate_cat
    )
    part_back = to_other_core(part_theirs)
    plate_theirs = to_other_core(plate_mine)
    first = tower_messages(0, table, bins, plate_mine, plate_theirs, tower_flip)
    own, *sums = core_sum(part_mine, part_back)
    back = [along_col(sums[d - 1], 0, d) for d in (1, 3, 2)]
    second = tower_messages(1, table, bins, plate_mine, plate_theirs, tower_flip)
    first_back = over_rows(first[0])
    second_back = [along_row(second[d], 0, d) for d in (1, 3, 2)]
    half = (HOME - CUT) * CLUSTER
    second_far = second[0][half:].astype(jnp.float32)
    for part in second_back:
        second_far = second_far + part[half:].astype(jnp.float32)
    second_far = second_far.astype(jnp.bfloat16)
    second_far = along_row(second_far, 1, 0)
    far = own[1024:].astype(jnp.float32)
    for part in back:
        far = far + part[1024:].astype(jnp.float32)
    far = far.astype(jnp.bfloat16)
    across = along_col(far, 1, 0)
    rest = ([own, *back], across, features, norm_gain.reshape(1, D), update_in, update_out)
    early = update(0, [first_back], *rest)
    return update(1, [early, second[0], *second_back, second_far], *rest)


def solution(mesh):
    placed = (
        P(("row", "col"), None),
        P(None, ("row", "col")),
        P(("row", "col"), None, None),
        P(),
        P(),
        P(),
        P(),
        P(),
    )
    return jax.shard_map(layer, mesh=mesh, in_specs=placed, out_specs=P(("row", "col"), None), check_vma=False)
```

```python
import jax
import jax.numpy as jnp
from jax import lax
from jax.experimental import pallas as pl
from jax.experimental.pallas import tpu as pltpu
from jax.sharding import PartitionSpec as P


D = 128
CLUSTER = 128
BINS = 8
SLOTS = 128
BLOCK = 8
HOME = 8
CUT = 4
MIB = 1024 * 1024


def live_count(index_ref):
    count = jnp.int32(0)
    for step in (128, 64, 32, 16, 8, 4, 2, 1):
        at = count + step
        inside = at <= SLOTS
        live = index_ref[0, jnp.minimum(at, SLOTS) - 1] >= 0
        count = jnp.where(inside & live, at, count)
    return count


def basis_of(level):
    one = jnp.ones((), jnp.bfloat16)
    zero = jnp.zeros((), jnp.bfloat16)
    level = level.astype(jnp.float32).astype(jnp.bfloat16)
    return [jnp.where(level == jnp.bfloat16(k), one, zero) for k in range(BINS)]


def plate_kernel(index_ref, bins_hbm, *refs):
    blocks_hbm, lines_hbm = refs[:8], refs[8:16]
    (weight_ref, mine_hbm, theirs_hbm, line_hbm, bins_ref, tower_ref, far_ref, acc_ref, out_ref,
     line_ref, sems, tower_sems, out_sems, line_sems) = refs[16:]
    row, col = index_ref[0, SLOTS], index_ref[1, SLOTS]
    row_z, row_x = row // 4, row % 4
    col_z, col_y, core = col // 8, (col // 2) % 4, col % 2

    def block_copy(j):
        source = ((row_z + 2 - j // 4) % 2) * 4 + (row_x + 4 - j % 4) % 4
        rows = pl.ds(pl.multiple_of(source * 1024, 1024), 1024)
        return pltpu.make_async_copy(blocks_hbm[j], tower_ref.at[rows], tower_sems.at[j])

    def line_copy(j):
        return pltpu.make_async_copy(lines_hbm[j], line_ref.at[pl.ds(j * 1024, 1024)], line_sems.at[j])

    line_out = pltpu.make_async_copy(line_ref, line_hbm, line_sems.at[8])

    for j in range(8):
        block_copy(j).start()
    for j in range(8):
        line_copy(j).start()
    count = live_count(index_ref)
    blocks = (count + BLOCK - 1) // BLOCK

    def bins_copy(block):
        part = pl.ds(block * BLOCK, BLOCK)
        return pltpu.make_async_copy(bins_hbm.at[part], bins_ref.at[part], sems.at[block])

    def start(block, _):
        bins_copy(block).start()
        return 0

    lax.fori_loop(0, blocks, start, 0)
    acc_ref[SLOTS] = jnp.zeros((CLUSTER, D), jnp.float32)

    def project(source, _):
        j = ((row_z + 2 - source // 4) % 2) * 4 + (row_x + 4 - source % 4) % 4
        at = pl.multiple_of(source * 1024, 1024)
        pltpu.make_async_copy(blocks_hbm[0], tower_ref.at[pl.ds(at, 1024)], tower_sems.at[j]).wait()
        for u in range(16):
            acc_ref[source * 16 + u] = jnp.zeros((CLUSTER, D), jnp.float32)
        for half in range(2):
            rows = tower_ref[pl.ds(at + half * 512, 512), :]
            for k in range(0, BINS, 2):
                both = jnp.dot(
                    rows, weight_ref[:, k * D : (k + 2) * D], preferred_element_type=jnp.float32
                ).astype(jnp.bfloat16)
                for u in range(4):
                    part = both[u * CLUSTER : (u + 1) * CLUSTER]
                    to = source * 8 + half * 4 + u
                    far_ref[to, k * CLUSTER : (k + 1) * CLUSTER, :] = part[:, :D]
                    far_ref[to, (k + 1) * CLUSTER : (k + 2) * CLUSTER, :] = part[:, D:]
        return 0

    lax.fori_loop(0, 8, project, 0)
    for j in range(8):
        line_copy(j).wait()
    line_out.start()

    def block_step(block, _):
        bins_copy(block).wait()
        for u in range(BLOCK):
            slot = block * BLOCK + u
            plate_at = index_ref[0, slot]
            plate_at = jnp.where(plate_at < 0, SLOTS, plate_at)
            tower_at = jnp.maximum(index_ref[1, slot], 0)
            basis = jnp.concatenate(basis_of(bins_ref[slot]), axis=1)
            message = jnp.dot(basis, far_ref[tower_at], preferred_element_type=jnp.float32)
            acc_ref[plate_at] += message
        return 0

    lax.fori_loop(0, blocks, block_step, 0)

    def out_copy(n):
        j = n % 8
        dest = (theirs_hbm, mine_hbm)[n // 8]
        return pltpu.make_async_copy(
            out_ref.at[pl.ds(n * 1024, 1024)], dest.at[pl.ds(j * 1024, 1024)], out_sems.at[n]
        )

    for n in range(16):
        j = n % 8
        side = 1 - core if n < 8 else core
        home = ((col_z + j % 2) % 2) * 8 + ((col_y + j // 2) % 4) * 2 + side
        for u in range(8):
            at = (n * 8 + u) * CLUSTER
            out_ref[at : at + CLUSTER, :] = acc_ref[home * 8 + u].astype(jnp.bfloat16)
        out_copy(n).start()
    for n in range(16):
        out_copy(n).wait()
    line_out.wait()


def tower_kernel(part, index_ref, bins_hbm, mine_hbm, theirs_hbm, weight_ref, *refs):
    out_refs = refs[: 1 if part == 0 else 8]
    bins_ref, plate_ref, acc_ref, near_a, near_b, slot_ref, from_ref, to_ref, sems, plate_sems = refs[len(out_refs) :]
    col = index_ref[1, SLOTS]
    col_z, col_y, core = col // 8, (col // 2) % 4, col % 2

    def block_copy(n):
        j = n % 8
        side = core if n < 8 else 1 - core
        source = ((col_z + 2 - j % 2) % 2) * 8 + ((col_y + 4 - j // 2) % 4) * 2 + side
        rows = pl.ds(pl.multiple_of(source * 1024, 1024), 1024)
        block = (mine_hbm, theirs_hbm)[n // 8].at[pl.ds(j * 1024, 1024)]
        return pltpu.make_async_copy(block, plate_ref.at[rows], plate_sems.at[n])

    for n in range(16):
        block_copy(n).start()
    live = live_count(index_ref)
    spare = acc_ref.shape[0] - 1

    first = CUT * part
    width = CUT if part == 0 else HOME - CUT
    for u in range(BLOCK):
        to_ref[u] = spare

    def pick(i, found):
        for u in range(BLOCK):
            slot = i * BLOCK + u
            tower_at = index_ref[1, slot]
            inner = tower_at % HOME
            slot_ref[found] = slot
            from_ref[found] = index_ref[0, slot]
            to_ref[found + BLOCK] = (tower_at // HOME) * width + inner - first
            mine = (tower_at >= 0) & (inner >= first) & (inner < first + width)
            found = found + jnp.where(mine, 1, 0)
        return found

    count = lax.fori_loop(0, (live + BLOCK - 1) // BLOCK, pick, jnp.int32(0))
    for u in range(BLOCK):
        slot_ref[count + u] = 0
        from_ref[count + u] = 0
        to_ref[count + u + BLOCK] = spare
    blocks = (count + BLOCK - 1) // BLOCK

    def start(block, _):
        for u in range(BLOCK):
            at = block * BLOCK + u
            pltpu.make_async_copy(bins_hbm.at[slot_ref[at]], bins_ref.at[at], sems.at[block]).start()
        return 0

    lax.fori_loop(0, blocks, start, 0)

    def zero(i, _):
        for u in range(8):
            acc_ref[i * 8 + u] = jnp.zeros((D, CLUSTER), jnp.float32)
        return 0

    lax.fori_loop(0, spare // 8, zero, 0)
    acc_ref[spare] = jnp.zeros((D, CLUSTER), jnp.float32)
    near_b[...] = jnp.zeros(near_b.shape, jnp.bfloat16)
    for n in range(16):
        block_copy(n).wait()

    def gather_near(base, near_ref):
        for u in range(BLOCK // 2):
            at = base + u
            rows = plate_ref[pl.ds(pl.multiple_of(from_ref[at] * CLUSTER, CLUSTER), CLUSTER), :]
            flipped = rows.T
            basis = basis_of(bins_ref[at])
            for k in range(0, BINS, 2):
                near = jnp.dot(
                    flipped, jnp.concatenate(basis[k : k + 2], axis=1), preferred_element_type=jnp.float32
                ).astype(jnp.bfloat16)
                for h in range(2):
                    near_ref[
                        u // 2, (k + h) * D : (k + h + 1) * D, (u % 2) * CLUSTER : (u % 2 + 1) * CLUSTER
                    ] = near[:, h * CLUSTER : (h + 1) * CLUSTER]

    def send_on(base, near_ref):
        for pair in range(BLOCK // 4):
            message = jnp.dot(weight_ref[...], near_ref[pair], preferred_element_type=jnp.float32)
            for u in range(2):
                acc_ref[to_ref[base + pair * 2 + u + BLOCK]] += message[:, u * CLUSTER : (u + 1) * CLUSTER]

    def block_step(block, _):
        base = block * BLOCK
        pltpu.make_async_copy(
            bins_hbm.at[pl.ds(0, BLOCK)], bins_ref.at[pl.ds(base, BLOCK)], sems.at[block]
        ).wait()
        gather_near(base, near_a)
        send_on(base - BLOCK // 2, near_b)
        gather_near(base + BLOCK // 2, near_b)
        send_on(base, near_a)
        return 0

    lax.fori_loop(0, blocks, block_step, 0)
    send_on(blocks * BLOCK - BLOCK // 2, near_b)

    row = index_ref[0, SLOTS]
    for j in range(8):
        home = j if part == 0 else ((row // 4 + j // 4) % 2) * 4 + (row % 4 + j % 4) % 4
        out_ref = out_refs[0 if part == 0 else j]
        for u in range(width):
            at = ((j * width if part == 0 else 0) + u) * CLUSTER
            out_ref[at : at + CLUSTER, :] = acc_ref[home * width + u].astype(jnp.bfloat16)


def add_kernel(mine_hbm, theirs_hbm, *refs):
    outs, (mine_ref, theirs_ref, sum_ref, in_sems, out_sems) = refs[:4], refs[4:]
    ins = []
    for j in range(4):
        rows = pl.ds(j * 2048, 2048)
        ins.append(
            (
                pltpu.make_async_copy(mine_hbm.at[rows], mine_ref.at[rows], in_sems.at[0, j]),
                pltpu.make_async_copy(theirs_hbm.at[rows], theirs_ref.at[rows], in_sems.at[1, j]),
            )
        )
    order = (1, 3, 2, 0)
    for j in order:
        for copy in ins[j]:
            copy.start()
    back = []
    for j in order:
        for copy in ins[j]:
            copy.wait()
        rows = pl.ds(j * 2048, 2048)
        total = mine_ref[rows, :].astype(jnp.float32) + theirs_ref[rows, :].astype(jnp.float32)
        sum_ref[rows, :] = total.astype(jnp.bfloat16)
        back.append(pltpu.make_async_copy(sum_ref.at[rows], outs[j], out_sems.at[j]))
        back[-1].start()
    for copy in back:
        copy.wait()


def updated_rows(flipped, rows, side_refs, features_ref, gain_ref, in_ref, last_ref):
    incoming = flipped.T
    for ref in side_refs:
        incoming += ref[rows, :].astype(jnp.float32)
    scale = lax.rsqrt(jnp.mean(incoming * incoming, axis=1, keepdims=True) + 1e-06)
    normed = (incoming * scale * gain_ref[...]).astype(jnp.bfloat16)
    features = features_ref[rows, :]
    mixed = jnp.dot(
        jnp.concatenate([features, normed], axis=1), in_ref[...], preferred_element_type=jnp.float32
    )
    hidden = (mixed / (1.0 + jnp.exp(-mixed))).astype(jnp.bfloat16)
    change = jnp.dot(hidden, last_ref[...], preferred_element_type=jnp.float32)
    return (features.astype(jnp.float32) + change).astype(jnp.bfloat16)


def early_kernel(arrived_ref, *refs):
    side_refs, (features_ref, gain_ref, in_ref, last_ref, out_hbm, out_ref, sem) = refs[:5], refs[5:]
    for c in range(CUT):
        rows = slice(c * CLUSTER, (c + 1) * CLUSTER)
        flipped = arrived_ref[0, rows, :].astype(jnp.float32)
        for r in range(1, 8):
            flipped += arrived_ref[r, rows, :].astype(jnp.float32)
        out_ref[rows, :] = updated_rows(flipped, rows, side_refs, features_ref, gain_ref, in_ref, last_ref)
    copy = pltpu.make_async_copy(out_ref, out_hbm.at[pl.ds(0, CUT * CLUSTER)], sem)
    copy.start()
    copy.wait()


def late_kernel(early_hbm, *refs):
    arrived_refs, side_refs, refs = refs[:8], refs[8:13], refs[13:]
    features_ref, gain_ref, in_ref, last_ref, out_hbm, out_ref, sem = refs
    for c in range(HOME - CUT):
        at = slice(c * CLUSTER, (c + 1) * CLUSTER)
        rows = slice((CUT + c) * CLUSTER, (CUT + c + 1) * CLUSTER)
        flipped = arrived_refs[0][at, :].astype(jnp.float32)
        for r in range(1, 8):
            flipped += arrived_refs[r][at, :].astype(jnp.float32)
        out_ref[at, :] = updated_rows(flipped, rows, side_refs, features_ref, gain_ref, in_ref, last_ref)
    copy = pltpu.make_async_copy(out_ref, out_hbm.at[pl.ds(CUT * CLUSTER, (HOME - CUT) * CLUSTER)], sem)
    copy.start()
    copy.wait()


SMEM = pl.BlockSpec(memory_space=pltpu.SMEM)
VMEM = pl.BlockSpec(memory_space=pltpu.VMEM)
HBM = pl.BlockSpec(memory_space=pltpu.HBM)
PARAMS = pltpu.CompilerParams(vmem_limit_bytes=50 * MIB)


def cost(flops, data):
    return pl.CostEstimate(flops=flops, bytes_accessed=data, transcendentals=0)


def plate_messages(pair_index, bins, blocks, lines, weight):
    half = jax.ShapeDtypeStruct((8192, D), jnp.bfloat16)
    return pl.pallas_call(
        plate_kernel,
        out_shape=(half, half, half),
        in_specs=[SMEM, HBM, *[HBM] * 16, VMEM],
        out_specs=(HBM, HBM, HBM),
        scratch_shapes=[
            pltpu.VMEM((SLOTS, CLUSTER, CLUSTER), jnp.int32),
            pltpu.VMEM((8192, D), jnp.bfloat16),
            pltpu.VMEM((64, BINS * CLUSTER, D), jnp.bfloat16),
            pltpu.VMEM((SLOTS + 1, CLUSTER, D), jnp.float32),
            pltpu.VMEM((16384, D), jnp.bfloat16),
            pltpu.VMEM((8192, D), jnp.bfloat16),
            pltpu.SemaphoreType.DMA((SLOTS // BLOCK,)),
            pltpu.SemaphoreType.DMA((8,)),
            pltpu.SemaphoreType.DMA((16,)),
            pltpu.SemaphoreType.DMA((9,)),
        ],
        compiler_params=PARAMS,
        cost_estimate=cost(25_000_000_000, 15_000_000),
        name="plate_messages",
    )(pair_index, bins, *blocks, *lines, weight)


def tower_messages(part, pair_index, bins, mine, theirs, weight):
    clusters = 8 * (CUT if part == 0 else HOME - CUT)
    outs = 1 if part == 0 else 8
    near = pltpu.VMEM((BLOCK // 4, BINS * D, 2 * CLUSTER), jnp.bfloat16)
    return pl.pallas_call(
        lambda *refs: tower_kernel(part, *refs),
        out_shape=[jax.ShapeDtypeStruct((clusters * CLUSTER // outs, D), jnp.bfloat16)] * outs,
        in_specs=[SMEM, HBM, HBM, HBM, VMEM],
        out_specs=[VMEM] * outs,
        scratch_shapes=[
            pltpu.VMEM((SLOTS, CLUSTER, CLUSTER), jnp.int32),
            pltpu.VMEM((16384, D), jnp.bfloat16),
            pltpu.VMEM((clusters + 1, D, CLUSTER), jnp.float32),
            near,
            near,
            pltpu.SMEM((SLOTS + BLOCK,), jnp.int32),
            pltpu.SMEM((SLOTS + BLOCK,), jnp.int32),
            pltpu.SMEM((SLOTS + 2 * BLOCK,), jnp.int32),
            pltpu.SemaphoreType.DMA((SLOTS // BLOCK,)),
            pltpu.SemaphoreType.DMA((16,)),
        ],
        compiler_params=pltpu.CompilerParams(vmem_limit_bytes=60 * MIB),
        cost_estimate=cost(15_000_000_000, 10_000_000),
    )(pair_index, bins, mine, theirs, weight)


def core_sum(mine, theirs):
    return pl.pallas_call(
        add_kernel,
        out_shape=tuple(jax.ShapeDtypeStruct((2048, D), jnp.bfloat16) for _ in range(4)),
        in_specs=[HBM, HBM],
        out_specs=tuple(HBM for _ in range(4)),
        scratch_shapes=[
            pltpu.VMEM((8192, D), jnp.bfloat16),
            pltpu.VMEM((8192, D), jnp.bfloat16),
            pltpu.VMEM((8192, D), jnp.bfloat16),
            pltpu.SemaphoreType.DMA((2, 4)),
            pltpu.SemaphoreType.DMA((4,)),
        ],
        compiler_params=PARAMS,
        cost_estimate=cost(2_000_000_000, 6_000_000),
        name="core_sum",
    )(mine, theirs)


def update(part, arrived, own_rows, across, features, gain, update_in, update_out):
    rows = (CUT if part == 0 else HOME - CUT) * CLUSTER
    return pl.pallas_call(
        early_kernel if part == 0 else late_kernel,
        out_shape=jax.ShapeDtypeStruct((1024, D), jnp.bfloat16),
        grid=(1,),
        in_specs=[HBM] * part
        + [VMEM] * (1 if part == 0 else 8)
        + [pl.BlockSpec((1024, D), lambda i: (0, 0))] * 4
        + [VMEM] * 5,
        out_specs=HBM,
        scratch_shapes=[pltpu.VMEM((rows, D), jnp.bfloat16), pltpu.SemaphoreType.DMA(())],
        input_output_aliases={0: 0} if part else {},
        compiler_params=pltpu.CompilerParams(vmem_limit_bytes=12 * MIB),
        cost_estimate=cost(2_000_000_000, 4_000_000),
    )(*arrived, *own_rows, across, features, gain, update_in, update_out)


def along_col(value, dz, dy):
    pairs = [
        (z * 8 + y * 2 + c, ((z + dz) % 2) * 8 + ((y + dy) % 4) * 2 + c)
        for z in range(2)
        for y in range(4)
        for c in range(2)
    ]
    return lax.ppermute(value, "col", pairs)


def along_row(value, dz, dx):
    pairs = [(z * 4 + x, ((z + dz) % 2) * 4 + (x + dx) % 4) for z in range(2) for x in range(4)]
    return lax.ppermute(value, "row", pairs)


def to_other_core(value):
    return lax.ppermute(value, "col", [(i, i ^ 1) for i in range(16)])


def over_rows(part):
    return lax.all_to_all(
        part.reshape(8, -1, D), "row", split_axis=0, concat_axis=0, tiled=True
    )


def layer(
    features, pair_index, bins, plate_weight, tower_weight, norm_gain, update_in, update_out
):
    place = jnp.stack([lax.axis_index("row"), lax.axis_index("col")]).astype(jnp.int32)
    table = jnp.concatenate([pair_index, jnp.broadcast_to(place[:, None], (2, SLOTS))], axis=1)
    plate_cat = plate_weight.reshape(BINS, D, D).transpose(1, 0, 2).reshape(D, BINS * D)
    tower_flip = tower_weight.T
    row_far = along_row(features, 1, 0)
    col_far = along_col(features, 1, 0)
    row_near = [along_row(features, 0, d) for d in (1, 3)]
    col_near = [along_col(features, 0, d) for d in (1, 3)]
    row_more = [along_row(row_far, 0, d) for d in (1, 3)]
    col_more = [along_col(col_far, 0, d) for d in (1, 3)]
    row_near.append(along_row(row_near[0], 0, 1))
    col_near.append(along_col(col_near[0], 0, 1))
    row_more.append(along_row(row_far, 0, 2))
    col_more.append(along_col(col_far, 0, 2))
    tower_blocks = [features, row_near[0], row_near[2], row_near[1], row_far, row_more[0], row_more[2], row_more[1]]
    lines = [features, col_far, col_near[0], col_more[0], col_near[2], col_more[2], col_near[1], col_more[1]]
    part_mine, part_theirs, plate_mine = plate_messages(
        table, bins, tower_blocks, lines, plate_cat
    )
    part_back = to_other_core(part_theirs)
    plate_theirs = to_other_core(plate_mine)
    first = tower_messages(0, table, bins, plate_mine, plate_theirs, tower_flip)
    own, *sums = core_sum(part_mine, part_back)
    back = [along_col(sums[d - 1], 0, d) for d in (1, 3, 2)]
    second = tower_messages(1, table, bins, plate_mine, plate_theirs, tower_flip)
    first_back = over_rows(first[0])
    second_back = [along_row(second[j], j // 4, j % 4) for j in (6, 5, 7, 4, 2, 1, 3)]
    far = own[1024:].astype(jnp.float32)
    for part in back:
        far = far + part[1024:].astype(jnp.float32)
    far = far.astype(jnp.bfloat16)
    across = along_col(far, 1, 0)
    rest = ([own, *back], across, features, norm_gain.reshape(1, D), update_in, update_out)
    early = update(0, [first_back], *rest)
    return update(1, [early, second[0], *second_back], *rest)


def solution(mesh):
    placed = (
        P(("row", "col"), None),
        P(None, ("row", "col")),
        P(("row", "col"), None, None),
        P(),
        P(),
        P(),
        P(),
        P(),
    )
    return jax.shard_map(layer, mesh=mesh, in_specs=placed, out_specs=P(("row", "col"), None), check_vma=False)
```
